32 devices in a mesh: dp: 4 (over y, z), ep: 8 (over x, core).
Axes of the slice: x: 4, y: 2, z: 2, core: 2. Of those that a mesh axis runs over, the one named last changes fastest.
The devices are a block of a 4x4x8 slice.
Arguments:
- h0: bfloat16 [32, 256, 2048], P(('dp', 'ep')), parts along dimension 0
- idx: int32 [32, 256, 8], P(('dp', 'ep')), parts along dimension 0
- slot: int32 [32, 256, 8], P(('dp', 'ep')), parts along dimension 0
- norm_attn: bfloat16 [2048], replicated
- wq: bfloat16 [2048, 2048], replicated
- wk: bfloat16 [2048, 2048], replicated
- wv: bfloat16 [2048, 2048], replicated
- wo: bfloat16 [2048, 2048], replicated
- norm_ffn: bfloat16 [2048], replicated
- w1: bfloat16 [2048, 8192], replicated
- w3: bfloat16 [2048, 8192], replicated
- w2: bfloat16 [8192, 2048], replicated
- norm_moe: bfloat16 [2048], replicated
- wr: bfloat16 [2048, 64], replicated
- ue1: bfloat16 [64, 2048, 1024], P('ep')
- ue3: bfloat16 [64, 2048, 1024], P('ep')
- ue2: bfloat16 [64, 1024, 2048], P('ep')
Outputs:
- output: bfloat16 [32, 256, 2048], P(('dp', 'ep')), parts along dimension 0
There are 4 independent parts. The reference program is written for one: setup_inputs(seed, part) draws one part's arguments, and reference() takes and returns one part's arrays. A program takes and returns all parts, laid end to end along the dimension named above; an argument that names none is the same for every part.
All inputs are finite; a program needn't handle non-finite values.
Results may differ from the reference program's by a relative error of at most 0.0105726.
Values are sent between devices in bfloat16 or wider.
A program may use at most 768 MiB of HBM per device.

```python
import jax
import jax.numpy as jnp
from jax import lax

D = 2048
HEADS = 16
KV_HEADS = 16
HEAD = 128
FF = 8192
EXPERTS = 64
TOP = 8
FE = 1024
SEQS_DEV = 1
SEQ = 256
EP = 8

TOKENS = SEQS_DEV * SEQ
CAP = 2 * TOKENS * TOP // EXPERTS
EPS = 1e-6
ROPE_BASE = 10000.0


def _w(key, shape, fan_in, scale=1.0):
    return (scale * fan_in ** -0.5 * jax.random.normal(key, shape, jnp.float32)).astype(jnp.bfloat16)


def _perms(key, count, size):
    return jax.vmap(lambda k: jax.random.permutation(k, size))(jax.random.split(key, count))


def setup_inputs(seed: int = 0, part: int = 0) -> dict:
    key = jax.random.PRNGKey(seed)
    ks = jax.random.split(key, 14)
    kp = jax.random.split(jax.random.fold_in(key, part), 4)
    kd = jax.random.split(jax.random.fold_in(jax.random.fold_in(key, part), 7), 4)
    avg = TOKENS * TOP // EXPERTS
    c = jnp.arange(TOKENS * TOP).reshape(TOKENS, TOP)
    half = TOKENS * TOP // 2
    low = c < half
    e0 = jnp.where(low, c % EXPERTS, (c - half) % (EXPERTS // 2))
    s0 = jnp.where(low, c // EXPERTS, avg // 2 + (c - half) // (EXPERTS // 2))
    shift = jax.random.randint(kd[2], (EP, EXPERTS), 0, CAP)
    tperm = jnp.broadcast_to(_perms(kd[3], EP, TOKENS)[:, :, None], (EP, TOKENS, TOP))
    idx = jnp.take_along_axis(jnp.broadcast_to(e0, (EP, TOKENS, TOP)), tperm, axis=1)
    slot = jnp.take_along_axis((s0[None] + shift[:, e0]) % CAP, tperm, axis=1)
    rshape = (EP * SEQS_DEV, SEQ, TOP)

    def nrm(k):
        return (1.0 + 0.2 * jax.random.normal(k, (D,), jnp.float32)).astype(jnp.bfloat16)

    return {
        'h0': jax.random.normal(kp[0], (EP * SEQS_DEV, SEQ, D), jnp.float32).astype(jnp.bfloat16),
        'idx': idx.reshape(rshape).astype(jnp.int32),
        'slot': slot.reshape(rshape).astype(jnp.int32),
        'norm_attn': nrm(ks[0]),
        'wq': _w(ks[1], (D, HEADS * HEAD), D),
        'wk': _w(ks[2], (D, KV_HEADS * HEAD), D),
        'wv': _w(ks[3], (D, KV_HEADS * HEAD), D),
        'wo': _w(ks[4], (HEADS * HEAD, D), HEADS * HEAD, 2.0),
        'norm_ffn': nrm(ks[5]),
        'w1': _w(ks[6], (D, FF), D),
        'w3': _w(ks[7], (D, FF), D),
        'w2': _w(ks[8], (FF, D), FF, 2.0),
        'norm_moe': nrm(ks[9]),
        'wr': _w(ks[10], (D, EXPERTS), D, 2.0),
        'ue1': _w(ks[11], (EXPERTS, D, FE), D),
        'ue3': _w(ks[12], (EXPERTS, D, FE), D),
        'ue2': _w(ks[13], (EXPERTS, FE, D), FE, 2.0),
    }


def _rms(x, w):
    xf = x.astype(jnp.float32)
    r = lax.rsqrt(jnp.mean(xf * xf, axis=-1, keepdims=True) + EPS)
    return (xf * r * w.astype(jnp.float32)).astype(jnp.bfloat16)


def _rope(x, cos, sin):
    h = HEAD // 2
    x1 = x[..., :h]
    x2 = x[..., h:]
    return jnp.concatenate([x1 * cos - x2 * sin, x2 * cos + x1 * sin], axis=-1)


def _dense_seq(h, na, wq, wk, wv, wo, nf, w1, w3, w2):
    f32 = jnp.float32
    bf = jnp.bfloat16
    pos = jnp.arange(SEQ).astype(f32)
    inv = ROPE_BASE ** (-2.0 * jnp.arange(HEAD // 2).astype(f32) / HEAD)
    ang = pos[:, None] * inv[None, :]
    cos = jnp.cos(ang)[:, None, :]
    sin = jnp.sin(ang)[:, None, :]
    x = _rms(h, na)
    q = _rope(jnp.dot(x, wq, preferred_element_type=f32).reshape(SEQ, HEADS, HEAD), cos, sin).astype(bf)
    k = _rope(jnp.dot(x, wk, preferred_element_type=f32).reshape(SEQ, KV_HEADS, HEAD), cos, sin).astype(bf)
    v = jnp.dot(x, wv, preferred_element_type=f32).astype(bf).reshape(SEQ, KV_HEADS, HEAD)
    q = q.reshape(SEQ, KV_HEADS, HEADS // KV_HEADS, HEAD)
    s = jnp.einsum('qgrd,kgd->grqk', q.astype(f32), k.astype(f32)) * HEAD ** -0.5
    causal = jnp.arange(SEQ)[:, None] >= jnp.arange(SEQ)[None, :]
    s = jnp.where(causal, s, -jnp.inf)
    p = jax.nn.softmax(s, axis=-1).astype(bf)
    o = jnp.einsum('grqk,kgd->qgrd', p.astype(f32), v.astype(f32)).astype(bf).reshape(SEQ, HEADS * HEAD)
    a = (h.astype(f32) + jnp.dot(o, wo, preferred_element_type=f32)).astype(bf)
    z = _rms(a, nf)
    hid = (jax.nn.silu(jnp.dot(z, w1, preferred_element_type=f32)) * jnp.dot(z, w3, preferred_element_type=f32)).astype(bf)
    return a.astype(f32) + jnp.dot(hid, w2, preferred_element_type=f32)


def reference(h0, idx, slot, norm_attn, wq, wk, wv, wo, norm_ffn, w1, w3, w2, norm_moe, wr, ue1, ue3, ue2):
    f32 = jnp.float32
    bf = jnp.bfloat16
    n = EP * TOKENS
    ix = idx.reshape(n, TOP)
    sl = slot.reshape(n, TOP)
    u = _rms(h0.reshape(n, D), norm_moe)
    logits = jnp.dot(u, wr, preferred_element_type=f32)
    g = jax.nn.softmax(jnp.take_along_axis(logits, ix, axis=1), axis=-1)
    rows = jnp.broadcast_to(jnp.arange(n, dtype=jnp.int32)[:, None], (n, TOP))
    src = rows // TOKENS
    tok = jnp.full((EP, EXPERTS, CAP), n, jnp.int32).at[src, ix, sl].set(rows)
    gb = jnp.zeros((EP, EXPERTS, CAP), f32).at[src, ix, sl].set(g)
    tok = tok.transpose(1, 0, 2).reshape(EXPERTS, EP * CAP)
    x = jnp.take(u, tok, axis=0, mode='fill', fill_value=0)

    def expert(args):
        xe, e1, e3, e2 = args
        hid = (jax.nn.silu(jnp.dot(xe, e1, preferred_element_type=f32)) * jnp.dot(xe, e3, preferred_element_type=f32)).astype(bf)
        return jnp.dot(hid, e2, preferred_element_type=f32).astype(bf)

    y = lax.map(expert, (x, ue1, ue3, ue2))
    gw = gb.transpose(1, 0, 2).reshape(EXPERTS, EP * CAP, 1)
    m = jnp.zeros((n, D), f32).at[tok.reshape(-1)].add((gw * y.astype(f32)).reshape(-1, D), mode='drop')
    dense = lax.map(lambda hs: _dense_seq(hs, norm_attn, wq, wk, wv, wo, norm_ffn, w1, w3, w2), h0)
    return (dense + m.reshape(EP * SEQS_DEV, SEQ, D)).astype(bf)
```

```python
import functools

import jax
import jax.numpy as jnp
from jax import lax
from jax.experimental import pallas as pl
from jax.experimental.pallas import tpu as pltpu
from jax.sharding import PartitionSpec as P

HEAD = 128
EPS = 1e-6
ROPE_BASE = 10000.0
MiB = 1 << 20
f32, bf16 = jnp.float32, jnp.bfloat16
MESH = pl.DeviceIdType.MESH


def _dot(a, b):
    return jnp.dot(a, b, preferred_element_type=f32)


def _norm(x, w):
    xf = x.astype(f32)
    r = lax.rsqrt(jnp.mean(xf * xf, axis=-1, keepdims=True) + EPS)
    return (xf * r * w.astype(f32)).astype(bf16)


def _loop(n, body):
    lax.fori_loop(0, n, lambda i, c: (body(i), c)[1], 0)


def _place(chips):
    me = lax.axis_index('ep')
    x, c = me // 2, me % 2
    return me, lambda dx, fc: lax.rem(x + dx, chips) * 2 + (lax.rem(c + fc, 2))


def _remote(src, dst, ssem, rsem, dev):
    return pltpu.make_async_remote_copy(src_ref=src, dst_ref=dst, send_sem=ssem, recv_sem=rsem,
                                        device_id={'ep': dev}, device_id_type=MESH)


def _greet(devs):
    bar = pltpu.get_barrier_semaphore()
    for d in devs:
        pl.semaphore_signal(bar, inc=1, device_id={'ep': d}, device_id_type=MESH)
    pl.semaphore_wait(bar, len(devs))


def _front_kernel(chips, k, cap, fb, hb,
                  h_ref, nm_ref, wrt_ref, idx_ref, slot_ref, na_ref, nf_ref, cos_ref, sin_ref,
                  wq_ref, wk_ref, wv_ref, wo_ref, ue1_ref, ue3_ref,
                  hid_ref, c_ref, a_ref, z_ref,
                  uall, maps, mall, xg, xa, acc, aring, bring, ering, hstage, cstage,
                  asem, esem, hsem, csem, usend, urecv, msend, mrecv):
    n = 2 * chips
    me, dev = _place(chips)
    t, d = h_ref.shape
    half = t // 2
    el = ue1_ref.shape[0]
    fe = ue1_ref.shape[2]
    wb = hb * HEAD
    ng = wq_ref.shape[1] // wb
    nf = fe // fb
    steps = el * nf
    deep = ering.shape[0]

    def attn_in(g, s):
        col = pl.ds(pl.multiple_of(g * wb, wb), wb)
        return [pltpu.make_async_copy(w.at[:, col], aring.at[s, i], asem.at[s, i])
                for i, w in enumerate((wq_ref, wk_ref, wv_ref))] + [
            pltpu.make_async_copy(wo_ref.at[col, :], bring.at[s], asem.at[s, 3])]

    def exp_in(i, s):
        e, j = i // nf, i % nf
        col = pl.ds(pl.multiple_of(j * fb, fb), fb)
        return [pltpu.make_async_copy(w.at[e, :, col], ering.at[s, q], esem.at[s, q])
                for q, w in enumerate((ue1_ref, ue3_ref))]

    for s in range(2):
        for cp in attn_in(s, s):
            cp.start()

    u = _norm(h_ref[...], nm_ref[...])
    uall[0] = u
    lt = lax.dot_general(wrt_ref[...], u, (((1,), (1,)), ((), ())), preferred_element_type=f32)
    ids = lax.broadcasted_iota(jnp.int32, lt.shape, 0)
    hits = [ids == idx_ref[j:j + 1, :] for j in range(k)]
    sel = [jnp.sum(jnp.where(h, lt, 0.0), axis=0, keepdims=True) for h in hits]
    top = functools.reduce(jnp.maximum, sel)
    ex = [jnp.exp(s - top) for s in sel]
    den = functools.reduce(jnp.add, ex)
    gate = jnp.zeros(lt.shape, f32)
    slot = jnp.full(lt.shape, -1.0, f32)
    for j in range(k):
        gate = jnp.where(hits[j], ex[j] / den, gate)
        slot = jnp.where(hits[j], slot_ref[j:j + 1, :].astype(f32), slot)
    maps[0] = slot
    maps[1] = gate
    xa[...] = _norm(h_ref[...], na_ref[...])
    acc[...] = jnp.zeros_like(acc)

    rel = [(p // 2, p % 2) for p in range(n)]
    others = [dev(*r) for r in rel[1:]]
    _greet(others)
    own = pl.ds(pl.multiple_of(me * el, el), el)
    mall[0] = maps[:, own, :]

    lo, hi = pl.ds(0, half), pl.ds(half, half)
    right, left, pair = dev(1, 0), dev(chips - 1, 0), dev(0, 1)
    hop = lambda i, a, b, rows, to: _remote(uall.at[a, rows], uall.at[b, rows], usend.at[i], urecv.at[i], to)
    r1, l1 = hop(0, 0, 2, lo, right), hop(1, 0, 6, hi, left)
    r2, l2 = hop(2, 0, 2, hi, right), hop(3, 0, 6, lo, left)
    p0 = hop(4, 0, 1, pl.ds(0, t), pair)
    ro, lo_ = hop(5, 2, 4, lo, right), hop(6, 6, 4, hi, left)
    p1, p3 = hop(7, 2, 3, pl.ds(0, t), pair), hop(8, 6, 7, pl.ds(0, t), pair)
    p2 = hop(9, 4, 5, pl.ds(0, t), pair)
    metas = [_remote(maps.at[:, pl.ds(pl.multiple_of(o * el, el), el), :], mall.at[p + 1],
                     msend.at[p], mrecv.at[p], o) for p, o in enumerate(others)]
    for m in metas:
        m.start()
    for m in (r1, l1, p0, r2, l2):
        m.start()
    for s in range(deep):
        for cp in exp_in(s, s):
            cp.start()

    def head_group(g):
        s = lax.rem(g, 2)
        for cp in attn_in(g, s):
            cp.wait()
        x = xa[...]
        q = _dot(x, aring[s, 0])
        kk = _dot(x, aring[s, 1])
        v = _dot(x, aring[s, 2]).astype(bf16)
        cos, sin = cos_ref[...], sin_ref[...]
        causal = lax.broadcasted_iota(jnp.int32, (t, t), 0) >= lax.broadcasted_iota(jnp.int32, (t, t), 1)
        outs = []
        for hd in range(hb):
            sl = slice(hd * HEAD, (hd + 1) * HEAD)
            qh = (q[:, sl] * cos + pltpu.roll(q[:, sl], HEAD // 2, 1) * sin).astype(bf16)
            kh = (kk[:, sl] * cos + pltpu.roll(kk[:, sl], HEAD // 2, 1) * sin).astype(bf16)
            sc = lax.dot_general(qh, kh, (((1,), (1,)), ((), ())), preferred_element_type=f32) * HEAD ** -0.5
            sc = jnp.where(causal, sc, -jnp.inf)
            e = jnp.exp(sc - jnp.max(sc, axis=-1, keepdims=True))
            pr = (e / jnp.sum(e, axis=-1, keepdims=True)).astype(bf16)
            outs.append(_dot(pr, v[:, sl]).astype(bf16))
        acc[...] += _dot(jnp.concatenate(outs, axis=1), bring[s])

        @pl.when(g + 2 < ng)
        def _():
            for cp in attn_in(g + 2, s):
                cp.start()

    _loop(ng, head_group)
    a = (h_ref[...].astype(f32) + acc[...]).astype(bf16)
    a_ref[...] = a
    z_ref[...] = _norm(a, nf_ref[...])

    r1.wait_recv()
    l1.wait_recv()
    ro.start()
    lo_.start()

    for m in metas:
        m.wait_recv()
    tm = jnp.concatenate([mall[p, 0] for p in range(n)] + [mall[p, 1] for p in range(n)], axis=0).T
    g1 = tm.astype(bf16)
    r = tm - g1.astype(f32)
    g2 = r.astype(bf16)
    g3 = (r - g2.astype(f32)).astype(bf16)
    lanes = lax.broadcasted_iota(jnp.int32, (t, el * cap), 1)
    lane_slot = lax.rem(lanes, cap).astype(f32)
    rows_i = lax.broadcasted_iota(jnp.int32, (tm.shape[1], el * cap), 0)
    cols_e = lax.broadcasted_iota(jnp.int32, (tm.shape[1], el * cap), 1) // cap

    def c_out(s, b):
        return pltpu.make_async_copy(cstage.at[b], c_ref.at[s], csem.at[b])

    def gates(s):
        b = lax.rem(s, 2)

        @pl.when(s >= 2)
        def _():
            c_out(s - 2, b).wait()

        pick_s = (rows_i == cols_e + s * el).astype(f32).astype(bf16)
        pick_g = (rows_i == cols_e + (s + n) * el).astype(f32).astype(bf16)
        hit = _dot(g1, pick_s) == lane_slot
        for i, g in enumerate((g1, g2, g3)):
            cstage[b, i * t:(i + 1) * t, :] = jnp.where(hit, _dot(g, pick_g), 0.0).astype(bf16)
        c_out(s, b).start()

    _loop(n, gates)
    for s in range(n - 2, n):
        c_out(s, s % 2).wait()

    slots_i = lax.broadcasted_iota(jnp.int32, (cap, t), 0).astype(f32)
    hs = n // 2
    rows = hs * cap

    def h_out(i, b, part):
        e, j = i // nf, i % nf
        return pltpu.make_async_copy(
            hstage.at[b], hid_ref.at[e, pl.ds(part * rows, rows), pl.ds(pl.multiple_of(j * fb, fb), fb)], hsem.at[b])

    def gather(part):
        def one(s):
            p = part * hs + s
            oh = jnp.concatenate([(slots_i == mall[p, 0, e:e + 1, :]).astype(f32).astype(bf16) for e in range(el)], axis=0)
            for c in range(0, d, 512):
                g = _dot(oh, uall[p, :, c:c + 512]).astype(bf16)
                for e in range(el):
                    xg[e, pl.ds(pl.multiple_of(s * cap, cap), cap), c:c + 512] = g[e * cap:(e + 1) * cap]
        _loop(hs, one)

    def hidden(part):
        def one(i):
            gi = part * steps + i
            s = lax.rem(gi, deep)
            b = lax.rem(i, 2)
            for cp in exp_in(i, s):
                cp.wait()
            x = xg[i // nf]
            h1 = _dot(x, ering[s, 0])
            h3 = _dot(x, ering[s, 1])

            @pl.when(i >= 2)
            def _():
                h_out(i - 2, b, part).wait()

            hstage[b] = (h1 * jax.nn.sigmoid(h1) * h3).astype(bf16)
            h_out(i, b, part).start()

            @pl.when(gi + deep < 2 * steps)
            def _():
                for cp in exp_in(lax.rem(i + deep, steps), s):
                    cp.start()

            if part == 0:
                @pl.when(i == (3 * steps) // 4)
                def _():
                    ro.wait_recv()
                    lo_.wait_recv()
                    p2.start()
        _loop(steps, one)
        for i in range(steps - 2, steps):
            h_out(i, i % 2, part).wait()

    r2.wait_recv()
    l2.wait_recv()
    p1.start()
    p3.start()
    p0.wait_recv()
    p1.wait_recv()
    gather(0)
    hidden(0)
    p3.wait_recv()
    p2.wait_recv()
    gather(1)
    hidden(1)
    for m in metas + [r1, l1, r2, l2, p0, ro, lo_, p1, p3, p2]:
        m.wait_send()


def _front(chips, cap, h, nm, wrt, idxt, slott, na, nf, cos, sin, wq, wk, wv, wo, ue1, ue3, fb=512, hb=4, deep=3):
    t, d = h.shape
    el, _, fe = ue1.shape
    n = 2 * chips
    k = idxt.shape[0]
    e = wrt.shape[0]
    vm, hbm = pl.BlockSpec(memory_space=pltpu.VMEM), pl.BlockSpec(memory_space=pl.ANY)
    dma = pltpu.SemaphoreType.DMA
    return pl.pallas_call(
        functools.partial(_front_kernel, chips, k, cap, fb, hb),
        in_specs=[vm] * 9 + [hbm] * 6,
        out_specs=[hbm, hbm, vm, vm],
        out_shape=(jax.ShapeDtypeStruct((el, n * cap, fe), bf16), jax.ShapeDtypeStruct((n, 3 * t, el * cap), bf16),
                   jax.ShapeDtypeStruct((t, d), bf16), jax.ShapeDtypeStruct((t, d), bf16)),
        scratch_shapes=[
            pltpu.VMEM((n, t, d), bf16), pltpu.VMEM((2, e, t), f32), pltpu.VMEM((n, 2, el, t), f32),
            pltpu.VMEM((el, n // 2 * cap, d), bf16), pltpu.VMEM((t, d), bf16), pltpu.VMEM((t, d), f32),
            pltpu.VMEM((2, 3, d, hb * HEAD), bf16), pltpu.VMEM((2, hb * HEAD, d), bf16),
            pltpu.VMEM((deep, 2, d, fb), bf16), pltpu.VMEM((2, n // 2 * cap, fb), bf16),
            pltpu.VMEM((2, 3 * t, el * cap), bf16),
            dma((2, 4)), dma((deep, 2)), dma((2,)), dma((2,)), dma((10,)), dma((10,)), dma((n - 1,)), dma((n - 1,)),
        ],
        compiler_params=pltpu.CompilerParams(vmem_limit_bytes=63 * MiB, collective_id=0, has_side_effects=True),
        name="front",
    )(h, nm, wrt, idxt, slott, na, nf, cos, sin, wq, wk, wv, wo, ue1, ue3)


def _back_kernel(chips, cap, cb, fb, z_ref, a_ref, hid_ref, c_hbm, ue2_ref, w1_ref, w3_ref, w2_ref, out_ref,
                 cbuf, hring, ering, y, p, got, part, relay, home, acc, fup, fdn,
                 csem, osem, fsem, dsend, drecv, rsend, rrecv):
    n = 2 * chips
    me, dev = _place(chips)
    t, d = z_ref.shape
    half = t // 2
    el, rows, fe = hid_ref.shape
    nch = d // cb
    deep = hring.shape[0]
    total = nch * el
    ff = w1_ref.shape[1]
    ng = ff // fb
    right, left, pair = dev(1, 0), dev(chips - 1, 0), dev(0, 1)

    def o_in(c, e, s):
        return [pltpu.make_async_copy(hid_ref.at[e], hring.at[s], osem.at[s, 0]),
                pltpu.make_async_copy(ue2_ref.at[e, :, pl.ds(c * cb, cb)], ering.at[s], osem.at[s, 1])]

    def f_in(g, s):
        col = pl.ds(pl.multiple_of(g * fb, fb), fb)
        return [pltpu.make_async_copy(w1_ref.at[:, col], fup.at[s, 0], fsem.at[s, 0]),
                pltpu.make_async_copy(w3_ref.at[:, col], fup.at[s, 1], fsem.at[s, 1]),
                pltpu.make_async_copy(w2_ref.at[col, :], fdn.at[s], fsem.at[s, 2])]

    for i in range(deep):
        for cp in o_in(0, i, i):
            cp.start()
    c_in = pltpu.make_async_copy(c_hbm, cbuf, csem)
    c_in.start()
    acc[...] = a_ref[...].astype(f32)
    _greet([right, left, pair])

    lo, hi = pl.ds(0, half), pl.ds(half, half)
    d2d = [_remote(p.at[1], got.at[c % 2], dsend.at[c], drecv.at[c], pair) for c in range(nch)]

    def hops(c):
        r = lambda i, src, dst, to: _remote(src, dst, rsend.at[c, i], rrecv.at[c, i], to)
        return (r(0, part.at[c, 1, lo], relay.at[c, 0], left), r(1, part.at[c, 1, hi], relay.at[c, 1], right),
                r(2, part.at[c, 0, hi], home.at[c, 0], left), r(3, part.at[c, 2, lo], home.at[c, 1], right),
                r(4, part.at[c, 0, lo], home.at[c, 2], left), r(5, part.at[c, 2, hi], home.at[c, 3], right))

    def chip_sums(c):
        d2d[c].wait()
        cs = slice(c * cb, (c + 1) * cb)
        for dx in (2, 1, 3):
            part[c, dx - 1] = p[0, dx] + got[c % 2, dx]
        acc[:, cs] += p[0, 0] + got[c % 2, 0]
        h = hops(c)
        for i in range(4):
            h[i].start()

    def relayed(c):
        h = hops(c)
        h[0].wait_recv()
        h[1].wait_recv()
        part[c, 0, lo] += relay[c, 0]
        part[c, 2, hi] += relay[c, 1]
        h[4].start()
        h[5].start()

    def arrived(c):
        h = hops(c)
        for i in range(2, 6):
            h[i].wait_recv()
        cs = slice(c * cb, (c + 1) * cb)
        acc[:half, cs] += home[c, 1] + home[c, 2]
        acc[half:, cs] += home[c, 0] + home[c, 3]

    for c in range(nch):
        def one(e, c=c):
            i = c * el + e
            s = lax.rem(i, deep)
            for cp in o_in(c, e, s):
                cp.wait()
            yy = _dot(hring[s], ering[s]).astype(bf16)
            for q in range(n):
                y[q, pl.ds(pl.multiple_of(e * cap, cap), cap), :] = yy[q * cap:(q + 1) * cap]

            @pl.when(e + deep < el)
            def _():
                for cp in o_in(c, e + deep, s):
                    cp.start()

            if c + 1 < nch:
                @pl.when(e + deep >= el)
                def _():
                    for cp in o_in(c + 1, e + deep - el, s):
                        cp.start()

        _loop(el, one)
        if c == 0:
            c_in.wait()
        if c >= 2:
            relayed(c - 2)
        if c >= 1:
            chip_sums(c - 1)

        def combine(q):
            r = _dot(cbuf[q], y[q])
            p[lax.rem(q, 2), q // 2] = r[:t] + r[t:2 * t] + r[2 * t:]

        _loop(n, combine)
        d2d[c].start()
        if c == 0:
            for s in range(2):
                for cp in f_in(s, s):
                    cp.start()

    events = {1: [lambda: relayed(nch - 2), lambda: chip_sums(nch - 1)], ng // 4: [lambda: arrived(0)],
              ng // 2: [lambda: arrived(1)], (5 * ng) // 8: [lambda: relayed(nch - 1)]}

    def group(g):
        s = lax.rem(g, 2)
        for cp in f_in(g, s):
            cp.wait()
        z = z_ref[...]
        h1 = _dot(z, fup[s, 0])
        h3 = _dot(z, fup[s, 1])
        acc[...] += _dot((h1 * jax.nn.sigmoid(h1) * h3).astype(bf16), fdn[s])

        @pl.when(g + 2 < ng)
        def _():
            for cp in f_in(g + 2, s):
                cp.start()

        for at, fs in events.items():
            @pl.when(g == at)
            def _(fs=fs):
                for f in fs:
                    f()

    _loop(ng, group)
    for c in range(2, nch):
        arrived(c)
    out_ref[...] = acc[...].astype(bf16)
    for c in range(nch):
        for h in hops(c):
            h.wait_send()


def _back(chips, cap, z, a, hid, c, ue2, w1, w3, w2, cb=512, fb=512, deep=4):
    t, d = z.shape
    el, rows, fe = hid.shape
    n = 2 * chips
    nch = d // cb
    vm, hbm = pl.BlockSpec(memory_space=pltpu.VMEM), pl.BlockSpec(memory_space=pl.ANY)
    dma = pltpu.SemaphoreType.DMA
    return pl.pallas_call(
        functools.partial(_back_kernel, chips, cap, cb, fb),
        in_specs=[vm] * 2 + [hbm] * 6,
        out_specs=vm,
        out_shape=jax.ShapeDtypeStruct((t, d), bf16),
        scratch_shapes=[
            pltpu.VMEM(c.shape, bf16), pltpu.VMEM((deep, rows, fe), bf16), pltpu.VMEM((deep, fe, cb), bf16),
            pltpu.VMEM((n, el * cap, cb), bf16), pltpu.VMEM((2, chips, t, cb), f32), pltpu.VMEM((2, chips, t, cb), f32),
            pltpu.VMEM((nch, 3, t, cb), f32), pltpu.VMEM((nch, 2, t // 2, cb), f32), pltpu.VMEM((nch, 4, t // 2, cb), f32),
            pltpu.VMEM((t, d), f32), pltpu.VMEM((2, 2, d, fb), bf16), pltpu.VMEM((2, fb, d), bf16),
            dma, dma((deep, 2)), dma((2, 3)), dma((nch,)), dma((nch,)), dma((nch, 6)), dma((nch, 6)),
        ],
        compiler_params=pltpu.CompilerParams(vmem_limit_bytes=63 * MiB, collective_id=1, has_side_effects=True),
        name="back",
    )(z, a, hid, c, ue2, w1, w3, w2)


def solution(mesh):
    G = mesh.shape['ep']

    def local(h0, idx, slot, na, wq, wk, wv, wo, nf, w1, w3, w2, nm, wr, ue1, ue3, ue2):
        b, s, d = h0.shape
        t = b * s
        k = idx.shape[-1]
        cap = 2 * t * k // (ue1.shape[0] * G)
        row = lambda w: w.reshape(1, d)
        ang = jnp.arange(s).astype(f32)[:, None] * (ROPE_BASE ** (-2.0 * jnp.arange(HEAD // 2).astype(f32) / HEAD))[None, :]
        cos, sin = jnp.cos(ang), jnp.sin(ang)
        hid, c, a, z = _front(G // 2, cap, h0.reshape(t, d), row(nm), wr.T, idx.reshape(t, k).T, slot.reshape(t, k).T,
                              row(na), row(nf), jnp.concatenate([cos, cos], 1), jnp.concatenate([-sin, sin], 1),
                              wq, wk, wv, wo, ue1, ue3)
        return _back(G // 2, cap, z, a, hid, c, ue2, w1, w3, w2).reshape(b, s, d)

    rows_spec = P(('dp', 'ep'))
    in_specs = (rows_spec,) * 3 + (P(),) * 11 + (P('ep'),) * 3
    return jax.shard_map(local, mesh=mesh, in_specs=in_specs, out_specs=rows_spec, check_vma=False)
```

```python
import functools

import jax
import jax.numpy as jnp
import numpy as np
from jax import lax
from jax.experimental import pallas as pl
from jax.experimental.pallas import tpu as pltpu
from jax.sharding import PartitionSpec as P

HEAD = 128
EPS = 1e-6
ROPE_BASE = 10000.0
MiB = 1 << 20
f32, bf16 = jnp.float32, jnp.bfloat16
MESH = pl.DeviceIdType.MESH


def _dot(a, b):
    return jnp.dot(a, b, preferred_element_type=f32)


def _norm(x, w):
    xf = x.astype(f32)
    r = lax.rsqrt(jnp.mean(xf * xf, axis=-1, keepdims=True) + EPS)
    return (xf * r * w).astype(bf16)


def _row(w_ref):
    w = w_ref[...].astype(f32)
    return jnp.concatenate([w[i:i + 1, :] for i in range(w.shape[0])], axis=1)


def _loop(n, body):
    lax.fori_loop(0, n, lambda i, c: (body(i), c)[1], 0)


def _sources(chips):
    far = list(range(2, chips - 1))
    near = [1, chips - 1]
    return [(0, 0), (0, 1)] + [(x, c) for c in (0, 1) for x in near] + [(x, c) for x in far for c in (0, 1)]


def _place(chips):
    me = lax.axis_index('ep')
    x, c = me // 2, me % 2
    return me, lambda dx, fc: lax.rem(x + dx, chips) * 2 + (lax.rem(c + fc, 2))


def _remote(src, dst, ssem, rsem, dev):
    return pltpu.make_async_remote_copy(src_ref=src, dst_ref=dst, send_sem=ssem, recv_sem=rsem,
                                        device_id={'ep': dev}, device_id_type=MESH)


def _front_kernel(chips, k, cap, fb, hb,
                  h_ref, nm_ref, wrt_ref, idx_ref, slot_ref, na_ref, nf_ref, cos_ref, sin_ref,
                  wq_ref, wk_ref, wv_ref, wo_ref, ue1_ref, ue3_ref,
                  hid_ref, c_ref, a_ref, z_ref,
                  uall, maps, mall, xg, xa, acc, aring, bring, ering, hstage, cstage,
                  asem, esem, hsem, csem, usend, urecv, msend, mrecv):
    n = 2 * chips
    me, dev = _place(chips)
    t, d = h_ref.shape
    half = t // 2
    el = ue1_ref.shape[0]
    fe = ue1_ref.shape[2]
    wb = hb * HEAD
    ng = wq_ref.shape[1] // wb
    nf = fe // fb
    deep = ering.shape[0]

    def attn_in(g, s):
        col = pl.ds(pl.multiple_of(g * wb, wb), wb)
        return [pltpu.make_async_copy(w.at[:, col], aring.at[s, i], asem.at[s, i])
                for i, w in enumerate((wq_ref, wk_ref, wv_ref))] + [
            pltpu.make_async_copy(wo_ref.at[col, :], bring.at[s], asem.at[s, 3])]

    def exp_in(e, j, s):
        col = pl.ds(pl.multiple_of(j * fb, fb), fb)
        return [pltpu.make_async_copy(w.at[e, :, col], ering.at[s, q], esem.at[s, q])
                for q, w in enumerate((ue1_ref, ue3_ref))]

    for s in range(2):
        for cp in attn_in(s, s):
            cp.start()

    rel = _sources(chips)
    others = [dev(*r) for r in rel[1:]]
    bar = pltpu.get_barrier_semaphore()
    for o in others:
        pl.semaphore_signal(bar, inc=1, device_id={'ep': o}, device_id_type=MESH)
    u = _norm(h_ref[...], _row(nm_ref))
    uall[0] = u
    pl.semaphore_wait(bar, len(others))

    lo, hi, whole = pl.ds(0, half), pl.ds(half, half), pl.ds(0, t)
    right, left, pair = dev(1, 0), dev(chips - 1, 0), dev(0, 1)
    hop = lambda i, a, b, rows, to: _remote(uall.at[a, rows], uall.at[b, rows], usend.at[i], urecv.at[i], to)
    r1, l1 = hop(0, 0, 2, lo, right), hop(1, 0, 3, hi, left)
    r2, l2 = hop(2, 0, 2, hi, right), hop(3, 0, 3, lo, left)
    p0 = hop(4, 0, 1, whole, pair)
    ro, lo_ = hop(5, 2, 6, lo, right), hop(6, 3, 6, hi, left)
    p1, p3 = hop(7, 2, 4, whole, pair), hop(8, 3, 5, whole, pair)
    p2 = hop(9, 6, 7, whole, pair)
    for m in (r1, l1, p0):
        m.start()

    lt = lax.dot_general(wrt_ref[...], u, (((1,), (1,)), ((), ())), preferred_element_type=f32)
    ids = lax.broadcasted_iota(jnp.int32, lt.shape, 0)
    hits = [ids == idx_ref[j:j + 1, :] for j in range(k)]
    sel = [jnp.sum(jnp.where(h, lt, 0.0), axis=0, keepdims=True) for h in hits]
    top = functools.reduce(jnp.maximum, sel)
    ex = [jnp.exp(s - top) for s in sel]
    den = functools.reduce(jnp.add, ex)
    gate = jnp.zeros(lt.shape, f32)
    slot = jnp.full(lt.shape, -1.0, f32)
    for j in range(k):
        gate = jnp.where(hits[j], ex[j] / den, gate)
        slot = jnp.where(hits[j], slot_ref[j:j + 1, :].astype(f32), slot)
    maps[0] = slot
    maps[1] = gate
    xa[...] = _norm(h_ref[...], _row(na_ref))
    acc[...] = jnp.zeros_like(acc)

    own = pl.ds(pl.multiple_of(me * el, el), el)
    mall[0] = maps[:, own, :]

    metas = [_remote(maps.at[:, pl.ds(pl.multiple_of(o * el, el), el), :], mall.at[p + 1],
                     msend.at[p], mrecv.at[p], o) for p, o in enumerate(others)]
    for m in metas + [r2, l2]:
        m.start()
    for s in range(deep):
        for cp in exp_in(s // nf, s % nf, s):
            cp.start()

    def head_group(g):
        s = lax.rem(g, 2)
        for cp in attn_in(g, s):
            cp.wait()
        x = xa[...]
        q = _dot(x, aring[s, 0])
        kk = _dot(x, aring[s, 1])
        v = _dot(x, aring[s, 2]).astype(bf16)
        cos, sin = cos_ref[...], sin_ref[...]
        causal = lax.broadcasted_iota(jnp.int32, (t, t), 0) >= lax.broadcasted_iota(jnp.int32, (t, t), 1)
        outs = []
        for hd in range(hb):
            sl = slice(hd * HEAD, (hd + 1) * HEAD)
            qh = (q[:, sl] * cos + pltpu.roll(q[:, sl], HEAD // 2, 1) * sin).astype(bf16)
            kh = (kk[:, sl] * cos + pltpu.roll(kk[:, sl], HEAD // 2, 1) * sin).astype(bf16)
            sc = lax.dot_general(qh, kh, (((1,), (1,)), ((), ())), preferred_element_type=f32) * HEAD ** -0.5
            sc = jnp.where(causal, sc, -jnp.inf)
            e = jnp.exp(sc - jnp.max(sc, axis=-1, keepdims=True))
            pr = (e / jnp.sum(e, axis=-1, keepdims=True)).astype(bf16)
            outs.append(_dot(pr, v[:, sl]).astype(bf16))
        acc[...] += _dot(jnp.concatenate(outs, axis=1), bring[s])

        @pl.when(g + 2 < ng)
        def _():
            for cp in attn_in(g + 2, s):
                cp.start()

    _loop(ng, head_group)
    a = (h_ref[...].astype(f32) + acc[...]).astype(bf16)
    a_ref[...] = a
    z_ref[...] = _norm(a, _row(nf_ref))

    r1.wait_recv()
    l1.wait_recv()
    ro.start()
    lo_.start()

    for m in metas:
        m.wait_recv()
    tm = jnp.concatenate([mall[p, 0] for p in range(n)] + [mall[p, 1] for p in range(n)], axis=0).T
    g1 = tm.astype(bf16)
    r = tm - g1.astype(f32)
    g2 = r.astype(bf16)
    g3 = (r - g2.astype(f32)).astype(bf16)
    lanes = lax.broadcasted_iota(jnp.int32, (t, el * cap), 1)
    lane_slot = lax.rem(lanes, cap).astype(f32)
    rows_i = lax.broadcasted_iota(jnp.int32, (tm.shape[1], el * cap), 0)
    cols_e = lax.broadcasted_iota(jnp.int32, (tm.shape[1], el * cap), 1) // cap

    def c_out(s, b):
        return pltpu.make_async_copy(cstage.at[b], c_ref.at[s], csem.at[b])

    def gates(s):
        b = lax.rem(s, 2)

        @pl.when(s >= 2)
        def _():
            c_out(s - 2, b).wait()

        pick_s = (rows_i == cols_e + s * el).astype(f32).astype(bf16)
        pick_g = (rows_i == cols_e + (s + n) * el).astype(f32).astype(bf16)
        hit = _dot(g1, pick_s) == lane_slot
        for i, g in enumerate((g1, g2, g3)):
            cstage[b, i * t:(i + 1) * t, :] = jnp.where(hit, _dot(g, pick_g), 0.0).astype(bf16)
        c_out(s, b).start()

    _loop(n, gates)
    for s in range(n - 2, n):
        c_out(s, s % 2).wait()

    slots_i = lax.broadcasted_iota(jnp.int32, (cap, t), 0).astype(f32)
    hs = n // 2
    rows = hs * cap

    def h_out(e, b, part):
        return pltpu.make_async_copy(hstage.at[b], hid_ref.at[e, pl.ds(part * rows, rows)], hsem.at[b])

    def gather(part, first, last):
        def one(s):
            p = part * hs + s
            oh = jnp.concatenate([(slots_i == mall[p, 0, e:e + 1, :]).astype(f32).astype(bf16) for e in range(el)], axis=0)
            for c in range(0, d, 512):
                g = _dot(oh, uall[p, :, c:c + 512]).astype(bf16)
                for e in range(el):
                    xg[e, pl.ds(pl.multiple_of(s * cap, cap), cap), c:c + 512] = g[e * cap:(e + 1) * cap]
        lax.fori_loop(first, last, lambda i, c: (one(i), c)[1], 0)

    def hidden(part):
        def one(i):
            gi = part * el * nf + i
            e, j = i // nf, lax.rem(i, nf)
            b, s = lax.rem(e, 2), lax.rem(gi, deep)
            for cp in exp_in(e, j, s):
                cp.wait()
            x = xg[e]

            @pl.when((e >= 2) & (j == 0))
            def _():
                h_out(e - 2, b, part).wait()

            h1 = _dot(x, ering[s, 0])
            h3 = _dot(x, ering[s, 1])
            hstage[b, :, pl.ds(pl.multiple_of(j * fb, fb), fb)] = (h1 * jax.nn.sigmoid(h1) * h3).astype(bf16)

            @pl.when(j == nf - 1)
            def _():
                h_out(e, b, part).start()

            @pl.when(gi + deep < 2 * el * nf)
            def _():
                nx = lax.rem(i + deep, el * nf)
                for cp in exp_in(nx // nf, lax.rem(nx, nf), s):
                    cp.start()

            if part == 0:
                @pl.when(i == (3 * el * nf) // 4)
                def _():
                    ro.wait_recv()
                    lo_.wait_recv()
                    p2.start()
        _loop(el * nf, one)
        for e in range(el - 2, el):
            h_out(e, e % 2, part).wait()

    p0.wait_recv()
    gather(0, 0, 2)
    r2.wait_recv()
    l2.wait_recv()
    p1.start()
    p3.start()
    gather(0, 2, hs)
    hidden(0)
    p1.wait_recv()
    p3.wait_recv()
    p2.wait_recv()
    gather(1, 0, hs)
    hidden(1)
    for m in metas + [r1, l1, r2, l2, p0, ro, lo_, p1, p3, p2]:
        m.wait_send()


def _front(chips, cap, h, nm, wrt, idxt, slott, na, nf, cos, sin, wq, wk, wv, wo, ue1, ue3, fb=512, hb=4, deep=4):
    t, d = h.shape
    el, _, fe = ue1.shape
    n = 2 * chips
    k = idxt.shape[0]
    e = wrt.shape[0]
    vm, hbm = pl.BlockSpec(memory_space=pltpu.VMEM), pl.BlockSpec(memory_space=pl.ANY)
    dma = pltpu.SemaphoreType.DMA
    return pl.pallas_call(
        functools.partial(_front_kernel, chips, k, cap, fb, hb),
        in_specs=[vm] * 9 + [hbm] * 6,
        out_specs=[hbm, hbm, vm, vm],
        out_shape=(jax.ShapeDtypeStruct((el, n * cap, fe), bf16), jax.ShapeDtypeStruct((n, 3 * t, el * cap), bf16),
                   jax.ShapeDtypeStruct((t, d), bf16), jax.ShapeDtypeStruct((t, d), bf16)),
        scratch_shapes=[
            pltpu.VMEM((n, t, d), bf16), pltpu.VMEM((2, e, t), f32), pltpu.VMEM((n, 2, el, t), f32),
            pltpu.VMEM((el, n // 2 * cap, d), bf16), pltpu.VMEM((t, d), bf16), pltpu.VMEM((t, d), f32),
            pltpu.VMEM((2, 3, d, hb * HEAD), bf16), pltpu.VMEM((2, hb * HEAD, d), bf16),
            pltpu.VMEM((deep, 2, d, fb), bf16), pltpu.VMEM((2, n // 2 * cap, fe), bf16),
            pltpu.VMEM((2, 3 * t, el * cap), bf16),
            dma((2, 4)), dma((deep, 2)), dma((2,)), dma((2,)), dma((10,)), dma((10,)), dma((n - 1,)), dma((n - 1,)),
        ],
        compiler_params=pltpu.CompilerParams(vmem_limit_bytes=63 * MiB, collective_id=0, has_side_effects=True),
        name="front",
    )(h, nm, wrt, idxt, slott, na, nf, cos, sin, wq, wk, wv, wo, ue1, ue3)


def _back_kernel(chips, cap, cuts, fb, z_ref, a_ref, hid_ref, c_hbm, ue2_ref, w1_ref, w3_ref, w2_ref, out_ref,
                 cbuf, hbuf, ering, y, p, got, part, relay, home, acc, fup, fdn,
                 csem, hsem, osem, fsem, dsend, drecv, rsend, rrecv):
    n = 2 * chips
    rel = _sources(chips)
    me, dev = _place(chips)
    t, d = z_ref.shape
    half = t // 2
    el, rows, fe = hid_ref.shape
    nch = len(cuts) - 1
    cols = [pl.ds(cuts[c], cuts[c + 1] - cuts[c]) for c in range(nch)]
    wide = [pl.ds(0, cuts[c + 1] - cuts[c]) for c in range(nch)]
    deep = ering.shape[0]
    ff = w1_ref.shape[1]
    ng = ff // fb
    right, left, pair = dev(1, 0), dev(chips - 1, 0), dev(0, 1)

    def o_in(c, e, s):
        return pltpu.make_async_copy(ue2_ref.at[e, :, cols[c]], ering.at[s, :, wide[c]], osem.at[s])

    def h_in(e):
        return pltpu.make_async_copy(hid_ref.at[e], hbuf.at[e], hsem.at[e])

    def f_in(g, s):
        col = pl.ds(pl.multiple_of(g * fb, fb), fb)
        return [pltpu.make_async_copy(w1_ref.at[:, col], fup.at[s, 0], fsem.at[s, 0]),
                pltpu.make_async_copy(w3_ref.at[:, col], fup.at[s, 1], fsem.at[s, 1]),
                pltpu.make_async_copy(w2_ref.at[col, :], fdn.at[s], fsem.at[s, 2])]

    for i in range(el):
        h_in(i).start()
        if i < deep:
            o_in(0, i, i).start()
    c_in = pltpu.make_async_copy(c_hbm, cbuf, csem)
    c_in.start()
    bar = pltpu.get_barrier_semaphore()
    for o in (right, left, pair):
        pl.semaphore_signal(bar, inc=1, device_id={'ep': o}, device_id_type=MESH)
    acc[...] = a_ref[...].astype(f32)
    pl.semaphore_wait(bar, 3)

    lo, hi = pl.ds(0, half), pl.ds(half, half)
    d2d = [_remote(p.at[1, :, :, wide[c]], got.at[c % 2, :, :, wide[c]], dsend.at[c], drecv.at[c], pair)
           for c in range(nch)]

    def hops(c):
        w = cols[c]
        r = lambda i, src, dst, to: _remote(src, dst, rsend.at[c, i], rrecv.at[c, i], to)
        return (r(0, part.at[1, lo, w], relay.at[0, :, w], left), r(1, part.at[1, hi, w], relay.at[1, :, w], right),
                r(2, part.at[0, hi, w], home.at[0, :, w], left), r(3, part.at[2, lo, w], home.at[1, :, w], right),
                r(4, part.at[0, lo, w], home.at[2, :, w], left), r(5, part.at[2, hi, w], home.at[3, :, w], right))

    def chip_sums(c):
        d2d[c].wait()
        w, v = cols[c], wide[c]
        for dx in (2, 1, 3):
            part[dx - 1, :, w] = p[0, dx, :, v] + got[c % 2, dx, :, v]
        acc[:, w] += p[0, 0, :, v] + got[c % 2, 0, :, v]
        for h in hops(c)[:4]:
            h.start()

    def relayed(c):
        h = hops(c)
        w = cols[c]
        h[0].wait_recv()
        h[1].wait_recv()
        part[0, lo, w] += relay[0, :, w]
        part[2, hi, w] += relay[1, :, w]
        h[4].start()
        h[5].start()

    def arrived(c):
        for h in hops(c)[2:]:
            h.wait_recv()
        w = cols[c]
        acc[lo, w] += home[1, :, w] + home[2, :, w]
        acc[hi, w] += home[0, :, w] + home[3, :, w]

    for c in range(nch):
        v = wide[c]

        def two(i, c=c, v=v):
            es = [2 * i, 2 * i + 1]
            ring = [lax.rem(c * el + e, deep) for e in es]
            for e, s in zip(es, ring):
                o_in(c, e, s).wait()
                if c == 0:
                    h_in(e).wait()
            for e, s in zip(es, ring):
                yy = _dot(hbuf[e], ering[s, :, v]).astype(bf16)
                for q in range(n):
                    y[q, pl.ds(pl.multiple_of(e * cap, cap), cap), v] = yy[q * cap:(q + 1) * cap]

            @pl.when(2 * i + deep < el)
            def _():
                for e, s in zip(es, ring):
                    o_in(c, e + deep, s).start()

            if c + 1 < nch:
                @pl.when(2 * i + deep >= el)
                def _():
                    for e, s in zip(es, ring):
                        o_in(c + 1, e + deep - el, s).start()

        _loop(el // 2, two)
        if c == 0:
            c_in.wait()
        if c >= 1:
            chip_sums(c - 1)
        for q in range(n):
            yq = y[q, :, v]
            dx, fc = rel[q]
            p[fc, dx, :, v] = _dot(cbuf[q, :t], yq) + _dot(cbuf[q, t:2 * t], yq) + _dot(cbuf[q, 2 * t:], yq)
        d2d[c].start()
        if c == 0:
            for s in range(2):
                for cp in f_in(s, s):
                    cp.start()
        if c == 1:
            relayed(0)

    events = {0: [functools.partial(chip_sums, nch - 1)]}
    for c, g in zip(range(1, nch), (0, 1, 3, 6)):
        events.setdefault((ng * g) // 16, []).append(functools.partial(relayed, c))
    soon = nch // 2
    for c in range(soon):
        events.setdefault((ng * (3 + 5 * c)) // 16, []).append(functools.partial(arrived, c))

    def group(g):
        s = lax.rem(g, 2)
        for cp in f_in(g, s):
            cp.wait()
        z = z_ref[...]
        h1 = _dot(z, fup[s, 0])
        h3 = _dot(z, fup[s, 1])
        acc[...] += _dot((h1 * jax.nn.sigmoid(h1) * h3).astype(bf16), fdn[s])

        @pl.when(g + 2 < ng)
        def _():
            for cp in f_in(g + 2, s):
                cp.start()

        for at, fs in events.items():
            @pl.when(g == at)
            def _(fs=fs):
                for f in fs:
                    f()

    _loop(ng, group)
    for c in range(soon, nch):
        arrived(c)
    out_ref[...] = acc[...].astype(out_ref.dtype)
    for c in range(nch):
        for h in hops(c):
            h.wait_send()


def _back(chips, cap, z, a, hid, c, ue2, w1, w3, w2, cb=512, first=256, fb=512, deep=4):
    t, d = z.shape
    el, rows, fe = hid.shape
    n = 2 * chips
    cuts = (0,) + tuple(range(first, d, cb)) + (d,)
    nch = len(cuts) - 1
    vm, hbm = pl.BlockSpec(memory_space=pltpu.VMEM), pl.BlockSpec(memory_space=pl.ANY)
    dma = pltpu.SemaphoreType.DMA
    return pl.pallas_call(
        functools.partial(_back_kernel, chips, cap, cuts, fb),
        in_specs=[vm] * 2 + [hbm] * 6,
        out_specs=vm,
        out_shape=jax.ShapeDtypeStruct((t, d), bf16),
        scratch_shapes=[
            pltpu.VMEM(c.shape, bf16), pltpu.VMEM(hid.shape, bf16), pltpu.VMEM((deep, fe, cb), bf16),
            pltpu.VMEM((n, el * cap, cb), bf16), pltpu.VMEM((2, chips, t, cb), f32), pltpu.VMEM((2, chips, t, cb), f32),
            pltpu.VMEM((3, t, d), f32), pltpu.VMEM((2, t // 2, d), f32), pltpu.VMEM((4, t // 2, d), f32),
            pltpu.VMEM((t, d), f32), pltpu.VMEM((2, 2, d, fb), bf16), pltpu.VMEM((2, fb, d), bf16),
            dma, dma((el,)), dma((deep,)), dma((2, 3)), dma((nch,)), dma((nch,)), dma((nch, 6)), dma((nch, 6)),
        ],
        compiler_params=pltpu.CompilerParams(vmem_limit_bytes=63 * MiB, collective_id=1, has_side_effects=True),
        name="back",
    )(z, a, hid, c, ue2, w1, w3, w2)


def solution(mesh):
    G = mesh.shape['ep']

    def local(h0, idx, slot, na, wq, wk, wv, wo, nf, w1, w3, w2, nm, wr, ue1, ue3, ue2):
        b, s, d = h0.shape
        t = b * s
        k = idx.shape[-1]
        cap = 2 * t * k // (ue1.shape[0] * G)
        row = lambda w: w.reshape(d // HEAD, HEAD)
        inv = np.float32(ROPE_BASE) ** (np.arange(HEAD // 2).astype(np.float32) * np.float32(-2.0 / HEAD))
        ang = np.arange(s).astype(np.float32)[:, None] * inv[None, :]
        cos, sin = np.cos(ang), np.sin(ang)
        hid, c, a, z = _front(G // 2, cap, h0.reshape(t, d), row(nm), wr.T, idx.reshape(t, k).T, slot.reshape(t, k).T,
                              row(na), row(nf), np.concatenate([cos, cos], 1), np.concatenate([-sin, sin], 1),
                              wq, wk, wv, wo, ue1, ue3)
        return _back(G // 2, cap, z, a, hid, c, ue2, w1, w3, w2).reshape(b, s, d)

    rows_spec = P(('dp', 'ep'))
    in_specs = (rows_spec,) * 3 + (P(),) * 11 + (P('ep'),) * 3
    return jax.shard_map(local, mesh=mesh, in_specs=in_specs, out_specs=rows_spec, check_vma=False)
```

```python
import functools

import jax
import jax.numpy as jnp
import numpy as np
from jax import lax
from jax.experimental import pallas as pl
from jax.experimental.pallas import tpu as pltpu
from jax.sharding import PartitionSpec as P

HEAD = 128
EPS = 1e-6
ROPE_BASE = 10000.0
MiB = 1 << 20
f32, bf16 = jnp.float32, jnp.bfloat16
MESH = pl.DeviceIdType.MESH


def _dot(a, b):
    return jnp.dot(a, b, preferred_element_type=f32)


def _norm(x, w):
    xf = x.astype(f32)
    r = lax.rsqrt(jnp.mean(xf * xf, axis=-1, keepdims=True) + EPS)
    return (xf * r * w).astype(bf16)


def _row(w_ref):
    w = w_ref[...].astype(f32)
    return jnp.concatenate([w[i:i + 1, :] for i in range(w.shape[0])], axis=1)


def _loop(n, body):
    lax.fori_loop(0, n, lambda i, c: (body(i), c)[1], 0)


def _sources(chips):
    far = list(range(2, chips - 1))
    near = [1, chips - 1]
    return [(0, 0), (0, 1)] + [(x, c) for c in (0, 1) for x in near] + [(x, c) for x in far for c in (0, 1)]


def _place(chips):
    me = lax.axis_index('ep')
    x, c = me // 2, me % 2
    return me, lambda dx, fc: lax.rem(x + dx, chips) * 2 + (lax.rem(c + fc, 2))


def _remote(src, dst, ssem, rsem, dev):
    return pltpu.make_async_remote_copy(src_ref=src, dst_ref=dst, send_sem=ssem, recv_sem=rsem,
                                        device_id={'ep': dev}, device_id_type=MESH)


def _front_kernel(chips, k, cap, fb, hb,
                  h_ref, nm_ref, wrt_ref, idx_ref, slot_ref, na_ref, nf_ref, cos_ref, sin_ref,
                  wq_ref, wk_ref, wv_ref, wo_ref, ue1_ref, ue3_ref,
                  hid_ref, c_ref, a_ref, z_ref,
                  uall, maps, mall, xg, xa, acc, aring, bring, ering, hstage, cstage,
                  asem, esem, hsem, csem, usend, urecv, msend, mrecv):
    n = 2 * chips
    me, dev = _place(chips)
    t, d = h_ref.shape
    half = t // 2
    el = ue1_ref.shape[0]
    fe = ue1_ref.shape[2]
    wb = hb * HEAD
    ng = wq_ref.shape[1] // wb
    nf = fe // fb
    deep = ering.shape[0]

    def attn_in(g, s):
        col = pl.ds(pl.multiple_of(g * wb, wb), wb)
        return [pltpu.make_async_copy(w.at[:, col], aring.at[s, i], asem.at[s, i])
                for i, w in enumerate((wq_ref, wk_ref, wv_ref))] + [
            pltpu.make_async_copy(wo_ref.at[col, :], bring.at[s], asem.at[s, 3])]

    def exp_in(e, j, s):
        col = pl.ds(j * fb, fb)
        return [pltpu.make_async_copy(w.at[e, :, col], ering.at[s, q], esem.at[s, q])
                for q, w in enumerate((ue1_ref, ue3_ref))]

    for s in range(2):
        for cp in attn_in(s, s):
            cp.start()

    rel = _sources(chips)
    others = [dev(*r) for r in rel[1:]]
    bar = pltpu.get_barrier_semaphore()
    for o in others:
        pl.semaphore_signal(bar, inc=1, device_id={'ep': o}, device_id_type=MESH)
    u = _norm(h_ref[...], _row(nm_ref))
    uall[0] = u
    pl.semaphore_wait(bar, len(others))

    lo, hi, whole = pl.ds(0, half), pl.ds(half, half), pl.ds(0, t)
    right, left, pair = dev(1, 0), dev(chips - 1, 0), dev(0, 1)
    hop = lambda i, a, b, rows, to: _remote(uall.at[a, rows], uall.at[b, rows], usend.at[i], urecv.at[i], to)
    r1, l1 = hop(0, 0, 2, lo, right), hop(1, 0, 3, hi, left)
    r2, l2 = hop(2, 0, 2, hi, right), hop(3, 0, 3, lo, left)
    p0 = hop(4, 0, 1, whole, pair)
    ro, lo_ = hop(5, 2, 6, lo, right), hop(6, 3, 6, hi, left)
    p1, p3 = hop(7, 2, 4, whole, pair), hop(8, 3, 5, whole, pair)
    p2 = hop(9, 6, 7, whole, pair)
    for m in (r1, l1, p0):
        m.start()

    lt = lax.dot_general(wrt_ref[...], u, (((1,), (1,)), ((), ())), preferred_element_type=f32)
    ids = lax.broadcasted_iota(jnp.int32, lt.shape, 0)
    hits = [ids == idx_ref[j:j + 1, :] for j in range(k)]
    sel = [jnp.sum(jnp.where(h, lt, 0.0), axis=0, keepdims=True) for h in hits]
    top = functools.reduce(jnp.maximum, sel)
    ex = [jnp.exp(s - top) for s in sel]
    den = functools.reduce(jnp.add, ex)
    gate = jnp.zeros(lt.shape, f32)
    slot = jnp.full(lt.shape, -1.0, f32)
    for j in range(k):
        gate = jnp.where(hits[j], ex[j] / den, gate)
        slot = jnp.where(hits[j], slot_ref[j:j + 1, :].astype(f32), slot)
    maps[0] = slot
    maps[1] = gate
    xa[...] = _norm(h_ref[...], _row(na_ref))
    acc[...] = jnp.zeros_like(acc)

    own = pl.ds(pl.multiple_of(me * el, el), el)
    mall[0] = maps[:, own, :]

    metas = [_remote(maps.at[:, pl.ds(pl.multiple_of(o * el, el), el), :], mall.at[p + 1],
                     msend.at[p], mrecv.at[p], o) for p, o in enumerate(others)]
    for m in metas + [r2, l2]:
        m.start()
    for s in range(deep):
        for cp in exp_in(s // nf, s % nf, s):
            cp.start()

    def head_group(g):
        s = lax.rem(g, 2)
        for cp in attn_in(g, s):
            cp.wait()
        x = xa[...]
        q = _dot(x, aring[s, 0])
        kk = _dot(x, aring[s, 1])
        v = _dot(x, aring[s, 2]).astype(bf16)
        cos, sin = cos_ref[...], sin_ref[...]
        causal = lax.broadcasted_iota(jnp.int32, (t, t), 0) >= lax.broadcasted_iota(jnp.int32, (t, t), 1)
        outs = []
        for hd in range(hb):
            sl = slice(hd * HEAD, (hd + 1) * HEAD)
            qh = (q[:, sl] * cos + pltpu.roll(q[:, sl], HEAD // 2, 1) * sin).astype(bf16)
            kh = (kk[:, sl] * cos + pltpu.roll(kk[:, sl], HEAD // 2, 1) * sin).astype(bf16)
            sc = lax.dot_general(qh, kh, (((1,), (1,)), ((), ())), preferred_element_type=f32) * HEAD ** -0.5
            sc = jnp.where(causal, sc, -jnp.inf)
            e = jnp.exp(sc - jnp.max(sc, axis=-1, keepdims=True))
            pr = (e * (1.0 / jnp.sum(e, axis=-1, keepdims=True))).astype(bf16)
            outs.append(_dot(pr, v[:, sl]).astype(bf16))
        acc[...] += _dot(jnp.concatenate(outs, axis=1), bring[s])

        @pl.when(g + 2 < ng)
        def _():
            for cp in attn_in(g + 2, s):
                cp.start()

    _loop(ng, head_group)
    a = (h_ref[...].astype(f32) + acc[...]).astype(bf16)
    a_ref[...] = a
    z_ref[...] = _norm(a, _row(nf_ref))

    r1.wait_recv()
    l1.wait_recv()
    ro.start()
    lo_.start()

    for m in metas:
        m.wait_recv()
    tm = jnp.concatenate([mall[p, 0] for p in range(n)] + [mall[p, 1] for p in range(n)], axis=0).T
    g1 = tm.astype(bf16)
    r = tm - g1.astype(f32)
    g2 = r.astype(bf16)
    g3 = (r - g2.astype(f32)).astype(bf16)
    lanes = lax.broadcasted_iota(jnp.int32, (t, el * cap), 1)
    lane_slot = lax.rem(lanes, cap).astype(f32)
    rows_i = lax.broadcasted_iota(jnp.int32, (tm.shape[1], el * cap), 0)
    cols_e = lax.broadcasted_iota(jnp.int32, (tm.shape[1], el * cap), 1) // cap

    def c_out(s, b):
        return pltpu.make_async_copy(cstage.at[b], c_ref.at[s], csem.at[b])

    def gates(s):
        b = lax.rem(s, 2)

        @pl.when(s >= 2)
        def _():
            c_out(s - 2, b).wait()

        pick_s = (rows_i == cols_e + s * el).astype(f32).astype(bf16)
        pick_g = (rows_i == cols_e + (s + n) * el).astype(f32).astype(bf16)
        hit = _dot(g1, pick_s) == lane_slot
        for i, g in enumerate((g1, g2, g3)):
            cstage[b, i * t:(i + 1) * t, :] = jnp.where(hit, _dot(g, pick_g), 0.0).astype(bf16)
        c_out(s, b).start()

    _loop(n, gates)
    for s in range(n - 2, n):
        c_out(s, s % 2).wait()

    slots_i = lax.broadcasted_iota(jnp.int32, (cap, t), 0).astype(f32)
    hs = n // 2
    rows = hs * cap

    def h_out(e, b, part):
        return pltpu.make_async_copy(hstage.at[b], hid_ref.at[e, pl.ds(part * rows, rows)], hsem.at[b])

    def gather(part, first, last):
        def one(s):
            p = part * hs + s
            oh = jnp.concatenate([(slots_i == mall[p, 0, e:e + 1, :]).astype(f32).astype(bf16) for e in range(el)], axis=0)
            for c in range(0, d, 512):
                g = _dot(oh, uall[p, :, c:c + 512]).astype(bf16)
                for e in range(el):
                    xg[e, pl.ds(pl.multiple_of(s * cap, cap), cap), c:c + 512] = g[e * cap:(e + 1) * cap]
        lax.fori_loop(first, last, lambda i, c: (one(i), c)[1], 0)

    def hidden(part):
        def one(e, refill):
            b = lax.rem(e, 2)
            ring = [lax.rem((part * el + e) * nf + j, deep) for j in range(nf)]

            @pl.when(e >= 2)
            def _():
                h_out(e - 2, b, part).wait()

            if part == 0:
                @pl.when(e == (3 * el) // 4)
                def _():
                    ro.wait_recv()
                    lo_.wait_recv()
                    p2.start()

            for j in range(nf):
                for cp in exp_in(e, j, ring[j]):
                    cp.wait()
            for j in range(nf):
                for c in range(0, fb, 256):
                    h1 = _dot(xg[e], ering[ring[j], 0, :, c:c + 256])
                    h3 = _dot(xg[e], ering[ring[j], 1, :, c:c + 256])
                    hstage[b, :, j * fb + c:j * fb + c + 256] = (h1 * jax.nn.sigmoid(h1) * h3).astype(bf16)
                if refill:
                    for cp in exp_in(lax.rem(e + deep // nf, el), j, ring[j]):
                        cp.start()
            h_out(e, b, part).start()

        ahead = deep // nf if part == 1 else 0
        lax.fori_loop(0, el - ahead, lambda e, c: (one(e, True), c)[1], 0)
        if ahead:
            lax.fori_loop(el - ahead, el, lambda e, c: (one(e, False), c)[1], 0)
        for e in range(el - 2, el):
            h_out(e, e % 2, part).wait()

    p0.wait_recv()
    gather(0, 0, 2)
    r2.wait_recv()
    l2.wait_recv()
    p1.start()
    p3.start()
    gather(0, 2, hs)
    hidden(0)
    p1.wait_recv()
    p3.wait_recv()
    p2.wait_recv()
    gather(1, 0, hs)
    hidden(1)
    for m in metas + [r1, l1, r2, l2, p0, ro, lo_, p1, p3, p2]:
        m.wait_send()


def _front(chips, cap, h, nm, wrt, idxt, slott, na, nf, cos, sin, wq, wk, wv, wo, ue1, ue3, fb=512, hb=4, deep=4):
    t, d = h.shape
    el, _, fe = ue1.shape
    n = 2 * chips
    k = idxt.shape[0]
    e = wrt.shape[0]
    vm, hbm = pl.BlockSpec(memory_space=pltpu.VMEM), pl.BlockSpec(memory_space=pl.ANY)
    dma = pltpu.SemaphoreType.DMA
    return pl.pallas_call(
        functools.partial(_front_kernel, chips, k, cap, fb, hb),
        in_specs=[vm] * 9 + [hbm] * 6,
        out_specs=[hbm, hbm, vm, vm],
        out_shape=(jax.ShapeDtypeStruct((el, n * cap, fe), bf16), jax.ShapeDtypeStruct((n, 3 * t, el * cap), bf16),
                   jax.ShapeDtypeStruct((t, d), bf16), jax.ShapeDtypeStruct((t, d), bf16)),
        scratch_shapes=[
            pltpu.VMEM((n, t, d), bf16), pltpu.VMEM((2, e, t), f32), pltpu.VMEM((n, 2, el, t), f32),
            pltpu.VMEM((el, n // 2 * cap, d), bf16), pltpu.VMEM((t, d), bf16), pltpu.VMEM((t, d), f32),
            pltpu.VMEM((2, 3, d, hb * HEAD), bf16), pltpu.VMEM((2, hb * HEAD, d), bf16),
            pltpu.VMEM((deep, 2, d, fb), bf16), pltpu.VMEM((2, n // 2 * cap, fe), bf16),
            pltpu.VMEM((2, 3 * t, el * cap), bf16),
            dma((2, 4)), dma((deep, 2)), dma((2,)), dma((2,)), dma((10,)), dma((10,)), dma((n - 1,)), dma((n - 1,)),
        ],
        compiler_params=pltpu.CompilerParams(vmem_limit_bytes=63 * MiB, collective_id=0, has_side_effects=True),
        name="front",
    )(h, nm, wrt, idxt, slott, na, nf, cos, sin, wq, wk, wv, wo, ue1, ue3)


def _back_kernel(chips, cap, cuts, fb, z_ref, a_ref, hid_ref, c_hbm, ue2_ref, w1_ref, w3_ref, w2_ref, out_ref,
                 cbuf, hbuf, ering, y, p, got, part, relay, home, acc, fup, fdn,
                 csem, hsem, osem, fsem, dsend, drecv, rsend, rrecv):
    n = 2 * chips
    rel = _sources(chips)
    me, dev = _place(chips)
    t, d = z_ref.shape
    half = t // 2
    el, rows, fe = hid_ref.shape
    nch = len(cuts) - 1
    cols = [pl.ds(cuts[c], cuts[c + 1] - cuts[c]) for c in range(nch)]
    wide = [pl.ds(0, cuts[c + 1] - cuts[c]) for c in range(nch)]
    deep = ering.shape[0]
    ff = w1_ref.shape[1]
    ng = ff // fb
    right, left, pair = dev(1, 0), dev(chips - 1, 0), dev(0, 1)

    def o_in(c, e, s):
        return pltpu.make_async_copy(ue2_ref.at[e, :, cols[c]], ering.at[s, :, wide[c]], osem.at[s])

    def h_in(e):
        return pltpu.make_async_copy(hid_ref.at[e], hbuf.at[e], hsem.at[e])

    def f_in(g, s):
        col = pl.ds(pl.multiple_of(g * fb, fb), fb)
        return [pltpu.make_async_copy(w1_ref.at[:, col], fup.at[s, 0], fsem.at[s, 0]),
                pltpu.make_async_copy(w3_ref.at[:, col], fup.at[s, 1], fsem.at[s, 1]),
                pltpu.make_async_copy(w2_ref.at[col, :], fdn.at[s], fsem.at[s, 2])]

    for i in range(el):
        h_in(i).start()
        if i < deep:
            o_in(0, i, i).start()
    c_in = pltpu.make_async_copy(c_hbm, cbuf, csem)
    c_in.start()
    bar = pltpu.get_barrier_semaphore()
    for o in (right, left, pair):
        pl.semaphore_signal(bar, inc=1, device_id={'ep': o}, device_id_type=MESH)
    acc[...] = a_ref[...].astype(f32)
    pl.semaphore_wait(bar, 3)

    lo, hi = pl.ds(0, half), pl.ds(half, half)
    d2d = [_remote(p.at[1, :, :, wide[c]], got.at[c % 2, :, :, wide[c]], dsend.at[c], drecv.at[c], pair)
           for c in range(nch)]

    def hops(c):
        w = cols[c]
        r = lambda i, src, dst, to: _remote(src, dst, rsend.at[c, i], rrecv.at[c, i], to)
        return (r(0, part.at[1, lo, w], relay.at[0, :, w], left), r(1, part.at[1, hi, w], relay.at[1, :, w], right),
                r(2, part.at[0, hi, w], home.at[0, :, w], left), r(3, part.at[2, lo, w], home.at[1, :, w], right),
                r(4, part.at[0, lo, w], home.at[2, :, w], left), r(5, part.at[2, hi, w], home.at[3, :, w], right))

    def chip_sums(c):
        d2d[c].wait()
        w, v = cols[c], wide[c]
        for dx in (2, 1, 3):
            part[dx - 1, :, w] = p[0, dx, :, v] + got[c % 2, dx, :, v]
        acc[:, w] += p[0, 0, :, v] + got[c % 2, 0, :, v]
        for h in hops(c)[:4]:
            h.start()

    def relayed(c):
        h = hops(c)
        w = cols[c]
        h[0].wait_recv()
        h[1].wait_recv()
        part[0, lo, w] += relay[0, :, w]
        part[2, hi, w] += relay[1, :, w]
        h[4].start()
        h[5].start()

    def arrived(c):
        for h in hops(c)[2:]:
            h.wait_recv()
        w = cols[c]
        acc[lo, w] += home[1, :, w] + home[2, :, w]
        acc[hi, w] += home[0, :, w] + home[3, :, w]

    sums, pass_on, home_in = chip_sums, relayed, arrived
    after_y = {2: [(pass_on, 0), (sums, 1)], 3: [(sums, 2)], 4: [(sums, 3), (pass_on, 2)],
               5: [(pass_on, 3), (sums, 4)]}
    after_c = {3: [(pass_on, 1)]}
    after_f = {2: [(sums, 5)], 3: [(pass_on, 4)], 4: [(home_in, 0)], 5: [(home_in, 1)], 6: [(home_in, 2)],
               7: [(home_in, 3)], 9: [(pass_on, 5)]}

    for c in range(nch):
        v = wide[c]

        def two(i, c=c, v=v):
            es = [2 * i, 2 * i + 1]
            ring = [lax.rem(c * el + e, deep) for e in es]
            for e, s in zip(es, ring):
                o_in(c, e, s).wait()
                if c == 0:
                    h_in(e).wait()
            for e, s in zip(es, ring):
                yy = _dot(hbuf[e], ering[s, :, v]).astype(bf16)
                for q in range(n):
                    y[q, pl.ds(pl.multiple_of(e * cap, cap), cap), v] = yy[q * cap:(q + 1) * cap]

            if c == 1:
                @pl.when(i == el // 4)
                def _():
                    chip_sums(0)

            @pl.when(2 * i + deep < el)
            def _():
                for e, s in zip(es, ring):
                    o_in(c, e + deep, s).start()

            if c + 1 < nch:
                @pl.when(2 * i + deep >= el)
                def _():
                    for e, s in zip(es, ring):
                        o_in(c + 1, e + deep - el, s).start()

        _loop(el // 2, two)
        if c == 0:
            c_in.wait()
        for f, i in after_y.get(c, ()):
            f(i)
        for q in range(n):
            yq = y[q, :, v]
            dx, fc = rel[q]
            p[fc, dx, :, v] = _dot(cbuf[q, :t], yq) + _dot(cbuf[q, t:2 * t], yq) + _dot(cbuf[q, 2 * t:], yq)
        d2d[c].start()
        if c == 0:
            for s in range(2):
                for cp in f_in(s, s):
                    cp.start()
        for f, i in after_c.get(c, ()):
            f(i)

    def group(g):
        s = lax.rem(g, 2)
        for cp in f_in(g, s):
            cp.wait()
        z = z_ref[...]
        h1 = _dot(z, fup[s, 0])
        h3 = _dot(z, fup[s, 1])
        acc[...] += _dot((h1 * jax.nn.sigmoid(h1) * h3).astype(bf16), fdn[s])

        @pl.when(g + 2 < ng)
        def _():
            for cp in f_in(g + 2, s):
                cp.start()

        for at, fs in after_f.items():
            @pl.when(g == (at * ng) // 16)
            def _(fs=fs):
                for f, i in fs:
                    f(i)

    _loop(ng, group)
    for c in range(4, nch):
        arrived(c)
    out_ref[...] = acc[...].astype(out_ref.dtype)
    for c in range(nch):
        for h in hops(c):
            h.wait_send()


def _back(chips, cap, z, a, hid, c, ue2, w1, w3, w2, cb=512, fb=512, deep=4):
    t, d = z.shape
    el, rows, fe = hid.shape
    n = 2 * chips
    cuts = tuple(i * d // 8 for i in (0, 1, 2, 3, 4, 6, 8))
    nch = len(cuts) - 1
    vm, hbm = pl.BlockSpec(memory_space=pltpu.VMEM), pl.BlockSpec(memory_space=pl.ANY)
    dma = pltpu.SemaphoreType.DMA
    return pl.pallas_call(
        functools.partial(_back_kernel, chips, cap, cuts, fb),
        in_specs=[vm] * 2 + [hbm] * 6,
        out_specs=vm,
        out_shape=jax.ShapeDtypeStruct((t, d), bf16),
        scratch_shapes=[
            pltpu.VMEM(c.shape, bf16), pltpu.VMEM(hid.shape, bf16), pltpu.VMEM((deep, fe, cb), bf16),
            pltpu.VMEM((n, el * cap, cb), bf16), pltpu.VMEM((2, chips, t, cb), f32), pltpu.VMEM((2, chips, t, cb), f32),
            pltpu.VMEM((3, t, d), f32), pltpu.VMEM((2, t // 2, d), f32), pltpu.VMEM((4, t // 2, d), f32),
            pltpu.VMEM((t, d), f32), pltpu.VMEM((2, 2, d, fb), bf16), pltpu.VMEM((2, fb, d), bf16),
            dma, dma((el,)), dma((deep,)), dma((2, 3)), dma((nch,)), dma((nch,)), dma((nch, 6)), dma((nch, 6)),
        ],
        compiler_params=pltpu.CompilerParams(vmem_limit_bytes=63 * MiB, collective_id=1, has_side_effects=True),
        name="back",
    )(z, a, hid, c, ue2, w1, w3, w2)


def solution(mesh):
    G = mesh.shape['ep']

    def local(h0, idx, slot, na, wq, wk, wv, wo, nf, w1, w3, w2, nm, wr, ue1, ue3, ue2):
        b, s, d = h0.shape
        t = b * s
        k = idx.shape[-1]
        cap = 2 * t * k // (ue1.shape[0] * G)
        row = lambda w: w.reshape(d // HEAD, HEAD)
        inv = np.float32(ROPE_BASE) ** (np.arange(HEAD // 2).astype(np.float32) * np.float32(-2.0 / HEAD))
        ang = np.arange(s).astype(np.float32)[:, None] * inv[None, :]
        cos, sin = np.cos(ang), np.sin(ang)
        hid, c, a, z = _front(G // 2, cap, h0.reshape(t, d), row(nm), wr.T, idx.reshape(t, k).T, slot.reshape(t, k).T,
                              row(na), row(nf), np.concatenate([cos, cos], 1), np.concatenate([-sin, sin], 1),
                              wq, wk, wv, wo, ue1, ue3)
        return _back(G // 2, cap, z, a, hid, c, ue2, w1, w3, w2).reshape(b, s, d)

    rows_spec = P(('dp', 'ep'))
    in_specs = (rows_spec,) * 3 + (P(),) * 11 + (P('ep'),) * 3
    return jax.shard_map(local, mesh=mesh, in_specs=in_specs, out_specs=rows_spec, check_vma=False)
```
